32 devices in a mesh: groups: 2 (over x), row: 16 (over z, y, core).
Axes of the slice: x: 2, y: 2, z: 4, core: 2. Of those that a mesh axis runs over, the one named last changes fastest.
Arguments:
- factor_b: bfloat16 [64, 131072], P(None, ('groups', 'row')), parts along dimension 1, may hold values from -12 to 12
- factor_c: bfloat16 [64, 131072], P(None, ('groups', 'row')), parts along dimension 1, may hold values from -12 to 12
- sample_j: int32 [262144], P(('groups', 'row')), parts along dimension 0, may hold values from 0 to 65535, as said below
- sample_k: int32 [16, 32, 512], P(None, ('groups', 'row')), parts along dimension 1, may hold values from 0 to 65535, as said below
- sample_weight: float32 [262144], P(('groups', 'row')), parts along dimension 0, may hold values from 0.5 to 3.5
- block_values: bfloat16 [32, 16, 4, 4, 128], P(('groups', 'row')), parts along dimension 0, may hold values from -24 to 24
- block_sample: int32 [32, 16, 4, 4], P(('groups', 'row')), parts along dimension 0, may hold values from 0 to 8191
- block_count: int32 [32, 16, 4, 4], P(('groups', 'row')), parts along dimension 0, may hold values from 0 to 128, as said below
Outputs:
- factor_new: bfloat16 [64, 16384], P(None, ('groups', 'row')), parts along dimension 1
- scales: float32 [128], P('groups'), parts along dimension 0
The draws below stay inside these ranges and needn't reach their ends.
There are 2 independent parts, one for each index of `groups`. The reference program is written for one: setup_inputs(seed, part) draws one part's arguments, and reference() takes and returns one part's arrays. A program takes and returns all parts, laid end to end along the dimension named above; each array names one. Nothing has to cross between parts.
Inputs may be any that keep to these rules, and one draw needn't show every extreme that they name: sample_j[s] lies in rows s // 8192 * 4096 to s // 8192 * 4096 + 4095. sample_k[d, e, i] is the third-mode index of sample d * 8192 + e * 512 + i and lies in rows e * 4096 to e * 4096 + 4095. `block_count`: 0 marks an empty slot; slot [p, p, 0, 0] holds 128 for every p.
All inputs are finite; a program needn't handle non-finite values.
Results may differ from the reference program's by a relative error of at most 0.0051.
Values may be sent and summed in bfloat16 or wider, within the bound.
No kernel may reach another device: no remote copies, remote signals or barrier semaphores. Data moves between devices by JAX's collectives and lax.ppermute only.
A program may use at most 64 MiB of HBM per device.

```python
import math
import jax
import jax.numpy as jnp
from jax import lax

R = 64
JD = 4096
KD = 4096
S_DEV = 8192
TD = 4
CT = 4
SPN = 512
S = 131072
J = 65536
K = 65536
I = 8192
N_ROW = 16


def factor_draw(key, total_rows):
    key_scale = jax.random.fold_in(key, 11)
    key_own = jax.random.fold_in(key, 12)
    key_spread = jax.random.fold_in(key, 14)
    column_scale = jnp.exp(jax.random.uniform(key_scale, (R, 1), minval=-math.log(1.5), maxval=math.log(1.5)))
    heavy_column = jax.random.randint(key_spread, (1, total_rows), 0, 128, dtype=jnp.int32) == 0
    spread_factor = jnp.where(heavy_column, 5.5, 0.8).astype(jnp.float32)
    own_part = jax.random.normal(key_own, (R, total_rows), dtype=jnp.float32)
    return (jnp.clip(own_part * spread_factor, -8.0, 8.0) * column_scale).astype(jnp.bfloat16)


def draw_factor_b(key, part):
    return factor_draw(jax.random.fold_in(key, 1), J)


def draw_factor_c(key, part):
    return factor_draw(jax.random.fold_in(key, 2), K)


def draw_sample_j(key, part):
    owner_block = jnp.arange(S, dtype=jnp.int32) // S_DEV
    offsets = jax.random.randint(jax.random.fold_in(key, 3), (S,), 0, JD, dtype=jnp.int32)
    return owner_block * JD + offsets


def draw_sample_k(key, part):
    holder = lax.broadcasted_iota(jnp.int32, (N_ROW, N_ROW, SPN), 1)
    offsets = jax.random.randint(jax.random.fold_in(key, 4), (N_ROW, N_ROW, SPN), 0, KD, dtype=jnp.int32)
    return holder * KD + offsets


def draw_sample_weight(key, part):
    device_pos = (jnp.arange(S, dtype=jnp.int32) // S_DEV).astype(jnp.float32)
    lift = jnp.sqrt(1.0 + 2.0 * device_pos / (N_ROW - 1))
    key_base = jax.random.fold_in(key, 5)
    base_weight = jnp.exp(jax.random.uniform(key_base, (S,), minval=-math.log(2.0), maxval=math.log(2.0)))
    return base_weight * lift


def draw_block_values(key, part):
    slot_shape = (N_ROW, N_ROW, TD, CT, 128)
    target = lax.broadcasted_iota(jnp.int32, slot_shape, 1).astype(jnp.float32)
    target_scale = 1.0 + 2.0 * target / (N_ROW - 1)
    key_noise = jax.random.fold_in(key, 6)
    noise_field = jax.random.normal(key_noise, slot_shape, dtype=jnp.float32)
    return (jnp.clip(noise_field, -8.0, 8.0) * target_scale).astype(jnp.bfloat16)


def draw_block_count(key, part):
    slot_shape = (N_ROW, N_ROW, TD, CT)
    source_ids = lax.broadcasted_iota(jnp.int32, slot_shape, 0)
    target_ids = lax.broadcasted_iota(jnp.int32, slot_shape, 1)
    tile_ids = lax.broadcasted_iota(jnp.int32, slot_shape, 2)
    slot_ids = lax.broadcasted_iota(jnp.int32, slot_shape, 3)
    fill_level = jax.random.randint(jax.random.fold_in(key, 7), (N_ROW,), 5, 9, dtype=jnp.int32)
    live_slot = jax.random.randint(jax.random.fold_in(key, 8), slot_shape, 0, 8, dtype=jnp.int32) < fill_level[None, :, None, None]
    most_live = 43 + 85 * source_ids // (N_ROW - 1)
    least_live = most_live // 2
    raw_count = jax.random.randint(jax.random.fold_in(key, 9), slot_shape, 0, 1 << 20, dtype=jnp.int32) % (most_live - least_live) + least_live + 1
    counted = jnp.where(live_slot, raw_count, jnp.zeros_like(raw_count))
    fixed_slot = (source_ids == target_ids) & (tile_ids == 0) & (slot_ids == 0)
    return jnp.where(fixed_slot, jnp.full_like(counted, 128), counted)


def place_ends(drawn, own_key, smallest, top_value):
    place = [jax.random.randint(jax.random.fold_in(own_key, axis), (), 0, length) for axis, length in enumerate(drawn.shape)]
    main_axis = drawn.shape.index(max(drawn.shape))
    beside = place[:main_axis] + [(place[main_axis] + 1) % drawn.shape[main_axis]] + place[main_axis + 1:]
    return drawn.at[tuple(place)].set(smallest).at[tuple(beside)].set(top_value)


def setup_inputs(seed: int = 0, part: int = 0) -> dict:
    key_list = jax.random.split(jax.random.key(seed), 9)
    own_keys = jax.random.split(jax.random.fold_in(key_list[8], part), 9)
    return {
        "factor_b": draw_factor_b(jax.random.fold_in(jax.random.fold_in(key_list[8], part), 71), part),
        "factor_c": draw_factor_c(jax.random.fold_in(jax.random.fold_in(key_list[8], part), 71), part),
        "sample_j": draw_sample_j(jax.random.fold_in(jax.random.fold_in(key_list[8], part), 71), part),
        "sample_k": draw_sample_k(jax.random.fold_in(jax.random.fold_in(key_list[8], part), 71), part),
        "sample_weight": draw_sample_weight(jax.random.fold_in(jax.random.fold_in(key_list[8], part), 71), part),
        "block_values": draw_block_values(jax.random.fold_in(jax.random.fold_in(key_list[8], part), 71), part),
        "block_sample": place_ends(jax.random.randint(own_keys[6], (N_ROW, N_ROW, TD, CT), 0, S_DEV), jax.random.fold_in(own_keys[6], 1), 0, S_DEV - 1).astype(jnp.int32),
        "block_count": draw_block_count(jax.random.fold_in(jax.random.fold_in(key_list[8], part), 71), part),
    }


def reference(factor_b, factor_c, sample_j, sample_k, sample_weight, block_values, block_sample, block_count):
    rank_width = factor_b.shape[0]
    b_columns = jnp.take(factor_b, sample_j, axis=1).astype(jnp.float32)
    c_columns = jnp.take(factor_c, sample_k.reshape(-1), axis=1).astype(jnp.float32)
    sketch = sample_weight[None, :] * b_columns * c_columns
    gram_matrix = jnp.dot(sketch, sketch.T, precision=lax.Precision.HIGHEST)
    live_total = jnp.sum(block_count.astype(jnp.float32))
    ridge = 0.05 * live_total / I
    system = gram_matrix / S + ridge * jnp.eye(rank_width, dtype=jnp.float32)
    lower_factor = jnp.linalg.cholesky(system)
    weighted = (sample_weight[None, :] * sketch).astype(jnp.bfloat16)
    positions = lax.broadcasted_iota(jnp.int32, block_values.shape, 4)
    masked = jnp.where(positions < block_count[..., None], block_values, jnp.zeros_like(block_values))
    owners = lax.broadcasted_iota(jnp.int32, block_sample.shape, 0) * S_DEV + block_sample
    picked = jnp.take(weighted, owners.reshape(-1).astype(jnp.int32), axis=1)
    picked = picked.reshape((rank_width,) + block_sample.shape)
    gathered = jnp.einsum('pqtcr,kpqtc->kqtr', masked.astype(jnp.float32), picked.astype(jnp.float32), precision=lax.Precision.HIGHEST).reshape(rank_width, -1)
    half_solved = lax.linalg.triangular_solve(lower_factor, gathered, left_side=True, lower=True)
    update = lax.linalg.triangular_solve(lower_factor, half_solved, left_side=True, lower=True, transpose_a=True)
    column_sums = lax.optimization_barrier(jnp.sum(update * update, axis=1))
    scales = jnp.sqrt(column_sums / I + 1e-06)
    return ((update / scales[:, None]).astype(jnp.bfloat16), scales)
```

```python
import jax
import jax.numpy as jnp
from jax import lax
from jax.sharding import PartitionSpec as P


def shards(
    factor_b, factor_c, sample_j, sample_k, sample_weight, block_values, block_sample, block_count
):
    rank_width = factor_b.shape[0]
    device_count = lax.axis_size("row")
    device_index = lax.axis_index("row")
    b_columns = jnp.take(factor_b, sample_j - device_index * factor_b.shape[1], axis=1)
    c_local = sample_k.reshape(-1) - device_index * factor_c.shape[1]
    c_outgoing = jnp.take(factor_c, c_local, axis=1).reshape(rank_width, device_count, -1)
    c_columns = lax.all_to_all(c_outgoing, "row", split_axis=1, concat_axis=1, tiled=True).reshape(
        rank_width, -1
    )
    sketch = sample_weight[None, :] * b_columns.astype(jnp.float32) * c_columns.astype(jnp.float32)
    gram_local = jnp.dot(sketch, sketch.T, precision=lax.Precision.HIGHEST)
    live_local = jnp.sum(block_count.astype(jnp.float32))
    live_row = jnp.full((1, rank_width), live_local, jnp.float32)
    pieces = lax.all_gather(jnp.concatenate([gram_local, live_row], axis=0), "row")
    summed = jnp.sum(pieces, axis=0)
    gram_matrix = summed[:rank_width]
    live_total = summed[rank_width, 0]
    weighted = (sample_weight[None, :] * sketch).astype(jnp.bfloat16)
    positions = lax.broadcasted_iota(jnp.int32, block_values.shape, 4)
    masked = jnp.where(
        positions < block_count[..., None], block_values, jnp.zeros_like(block_values)
    )[0]
    tile_count = masked.shape[1]
    slot_count = masked.shape[2]
    weighted_rows = weighted.T
    picked = jnp.take(weighted_rows, block_sample.reshape(-1), axis=0)
    picked = picked.reshape(device_count, tile_count, slot_count, rank_width)
    values_in, rows_in = (
        lax.all_to_all(
            masked.reshape(device_count, -1), "row", split_axis=0, concat_axis=0, tiled=True
        ),
        lax.all_to_all(
            picked.reshape(device_count, -1), "row", split_axis=0, concat_axis=0, tiled=True
        ),
    )
    gathered = jnp.einsum(
        "stcr,stck->ktr",
        values_in.reshape(masked.shape),
        rows_in.reshape(picked.shape),
        preferred_element_type=jnp.float32,
    ).reshape(rank_width, -1)
    total_rows = gathered.shape[1] * device_count
    total_samples = sketch.shape[1] * device_count
    ridge = 0.05 * live_total / total_rows
    system = gram_matrix / total_samples + ridge * jnp.eye(rank_width, dtype=jnp.float32)
    lower_factor = jnp.linalg.cholesky(system)
    half_solved = lax.linalg.triangular_solve(lower_factor, gathered, left_side=True, lower=True)
    update = lax.linalg.triangular_solve(
        lower_factor, half_solved, left_side=True, lower=True, transpose_a=True
    )
    column_sums = jnp.sum(lax.all_gather(jnp.sum(update * update, axis=1), "row"), axis=0)
    scales = jnp.sqrt(column_sums / total_rows + 1e-06)
    return ((update / scales[:, None]).astype(jnp.bfloat16), scales)


def solution(mesh):
    in_specs = (
        P(None, ("groups", "row")),
        P(None, ("groups", "row")),
        P(("groups", "row")),
        P(None, ("groups", "row"), None),
        P(("groups", "row")),
        P(("groups", "row"), None, None, None, None),
        P(("groups", "row"), None, None, None),
        P(("groups", "row"), None, None, None),
    )
    out_specs = (P(None, ("groups", "row")), P("groups"))
    return jax.shard_map(shards, mesh=mesh, in_specs=in_specs, out_specs=out_specs, check_vma=False)
```

```python
import functools

import jax
import jax.numpy as jnp
from jax import lax
from jax.experimental import pallas as pl
from jax.experimental.pallas import tpu as pltpu
from jax.sharding import PartitionSpec as P

LANES = 128
HIGHEST = lax.Precision.HIGHEST
VMEM = pl.BlockSpec(memory_space=pltpu.VMEM)
SMEM = pl.BlockSpec(memory_space=pltpu.SMEM)
OVER_ROWS = (((0,), (0,)), ((), ()))


def lane_index(shape):
    return lax.broadcasted_iota(jnp.int32, shape, 1)


def fill_table(factor_ref, table_ref):
    columns = factor_ref.shape[1]

    def step(chunk, carry):
        start = pl.multiple_of(chunk * LANES, LANES)
        block = factor_ref[:, pl.ds(start, LANES)].astype(jnp.float32)
        table_ref[pl.ds(start, LANES), :] = jnp.concatenate([block, block], axis=0).T
        return carry

    lax.fori_loop(0, columns // LANES, step, 0)


def gather_pairs(base_ref, index_ref, table_ref, rows_ref, span):
    half = span // 2
    step_rows = min(32, half)
    low = lane_index((1, LANES)) < LANES // 2
    base = base_ref[0]

    def step(q, carry):
        row = q * step_rows
        first = row + lax.div(row, half) * half
        for u in range(step_rows):
            a = index_ref[first + u] - base
            b = index_ref[first + (u + half)] - base
            rows_ref[pl.ds(row + u, 1), :] = jnp.where(
                low, table_ref[pl.ds(a, 1), :], table_ref[pl.ds(b, 1), :]
            )
        return carry

    lax.fori_loop(0, rows_ref.shape[0] // step_rows, step, 0)


def outgoing_kernel(base_ref, index_ref, factor_ref, out_ref, table_ref, rows_ref, *, span):
    fill_table(factor_ref, table_ref)
    gather_pairs(base_ref, index_ref, table_ref, rows_ref, span)
    out_ref[...] = rows_ref[...].astype(jnp.bfloat16)


def weighted_b_kernel(base_ref, index_ref, weight_ref, factor_ref, out_ref, table_ref, *, span):
    half = span // 2
    fill_table(factor_ref, table_ref)
    gather_pairs(base_ref, index_ref, table_ref, out_ref, span)
    turned = weight_ref[...].T
    low = lane_index((half, LANES)) < LANES // 2
    for e in range(out_ref.shape[0] // half):
        weights = jnp.where(low, turned[:, 2 * e : 2 * e + 1], turned[:, 2 * e + 1 : 2 * e + 2])
        out_ref[e * half : (e + 1) * half, :] = out_ref[e * half : (e + 1) * half, :] * weights


def sketch_kernel(
    sample_ref, count_ref, weight_ref, wb_ref, c_ref, values_ref, out_ref, sketch_ref, values32_ref, *, span
):
    half = span // 2
    total_rows = wb_ref.shape[0]
    devices, _, _ = out_ref.shape
    blocks = values_ref.shape[0] // devices
    chunk = min(512, total_rows)

    def gram_step(q, acc):
        start = pl.multiple_of(q * chunk, chunk)
        x = wb_ref[pl.ds(start, chunk), :] * c_ref[pl.ds(start, chunk), :].astype(jnp.float32)
        sketch_ref[pl.ds(start, chunk), :] = x
        high = x.astype(jnp.bfloat16)
        rest = (x - high.astype(jnp.float32)).astype(jnp.bfloat16)
        both = jnp.concatenate([high, rest], axis=1)
        return acc + lax.dot_general(high, both, OVER_ROWS, preferred_element_type=jnp.float32)

    acc = lax.fori_loop(
        0, total_rows // chunk, gram_step, jnp.zeros((LANES, 2 * LANES), jnp.float32)
    )
    rank = LANES // 2
    cross = acc[:, LANES:]
    full = acc[:, :LANES] + cross + cross.T
    gram = full[:rank] + pltpu.roll(full[rank:], rank, 1)
    low = lane_index((1, LANES)) < rank
    packed = jnp.where(low, gram[: rank // 2], pltpu.roll(gram[rank // 2 :], rank, 1))
    lane = lane_index((1, LANES))
    values32_ref[...] = values_ref[...].astype(jnp.float32)

    def count_step(q, total):
        for u in range(blocks):
            total = total + count_ref[q * blocks + u]
        return total

    live = lax.fori_loop(0, devices, count_step, jnp.int32(0)).astype(jnp.float32)

    def pick_step(q, carry):
        for u in range(blocks):
            j = q * blocks + u
            s = sample_ref[j]
            e = lax.div(s, span)
            i = s - e * span
            upper = i >= half
            row = e * half + jnp.where(upper, i - half, i)
            scaled = sketch_ref[pl.ds(row, 1), :] * weight_ref[s]
            picked = jnp.where(upper, pltpu.roll(scaled, rank, 1), scaled)
            rounded = picked.astype(jnp.bfloat16).astype(jnp.float32)
            out_ref[q, blocks + u : blocks + u + 1, :] = jnp.where(low, rounded, live)
            value_row = values32_ref[pl.ds(j, 1), :]
            out_ref[q, u : u + 1, :] = jnp.where(lane < count_ref[j], value_row, 0.0)
        out_ref[q, 2 * blocks :, :] = packed
        return carry

    lax.fori_loop(0, devices, pick_step, 0)


def solve_kernel(in_ref, update_ref, sums_ref, *, tiles, slots, total_rows, total_samples):
    devices = in_ref.shape[0]
    rank = LANES // 2
    blocks = tiles * slots
    summed = in_ref[0, 2 * blocks :, :]
    live_row = in_ref[0, blocks : blocks + 1, :]
    for p in range(1, devices):
        summed = summed + in_ref[p, 2 * blocks :, :]
        live_row = live_row + in_ref[p, blocks : blocks + 1, :]
    gram = jnp.concatenate([summed, pltpu.roll(summed, rank, 1)], axis=0)
    ridge = 0.05 * pltpu.roll(live_row, rank, 1)[:, 0:1] / total_rows
    lane = lane_index((rank, LANES))
    sub = lax.broadcasted_iota(jnp.int32, (rank, LANES), 0)
    state = gram / total_samples + jnp.where(lane == sub, ridge, 0.0)
    lane_row = lane_index((1, LANES))
    for k in range(rank):
        pivot = 1.0 / state[k : k + 1, k : k + 1]
        row = jnp.where(lane_row == k, 1.0, state[k : k + 1, :]) * pivot
        column = state[:, k : k + 1]
        rest = jnp.where(lane == k, 0.0, state)
        state = jnp.where(sub == k, row, rest - column * row)
    inverse = state[:, :rank]
    values = in_ref[:, :blocks, :].reshape(devices * blocks, LANES).astype(jnp.bfloat16)
    rows = in_ref[:, blocks : 2 * blocks, :].reshape(devices * blocks, LANES)
    wide = lane_index(rows.shape)
    doubled = jnp.where(wide < rank, rows, pltpu.roll(rows, rank, 1))
    tile_of = lax.div(
        lax.rem(lax.broadcasted_iota(jnp.int32, rows.shape, 0), blocks), slots
    )
    parts = []
    for g in range(0, tiles, 2):
        wanted = jnp.where(wide < rank, g, g + 1)
        left = jnp.where(tile_of == wanted, doubled, 0.0).astype(jnp.bfloat16)
        both = lax.dot_general(left, values, OVER_ROWS, preferred_element_type=jnp.float32)
        parts += [both[:rank], both[rank:]]
    gathered = jnp.concatenate(parts[:tiles], axis=1)
    update = jnp.dot(inverse, gathered, precision=HIGHEST, preferred_element_type=jnp.float32)
    update_ref[...] = update
    column_sums = jnp.sum(update * update, axis=1, keepdims=True)
    turned = jnp.broadcast_to(
        jnp.concatenate([column_sums, column_sums], axis=0), (LANES, LANES)
    ).T
    for p in range(devices):
        sums_ref[p] = turned[:8]


def scale_kernel(sums_ref, update_ref, out_ref, scales_ref, *, total_rows):
    rank = update_ref.shape[0]
    summed = sums_ref[0]
    for p in range(1, sums_ref.shape[0]):
        summed = summed + sums_ref[p]
    scales = jnp.sqrt(summed / total_rows + 1e-06)
    scales_ref[...] = scales
    column = jnp.broadcast_to(scales[0:1], (LANES, LANES)).T[:rank, 0:1]
    out_ref[...] = (update_ref[...] / column).astype(jnp.bfloat16)


def shape(dims, dtype):
    return jax.ShapeDtypeStruct(dims, dtype)


def shards(
    factor_b, factor_c, sample_j, sample_k, sample_weight, block_values, block_sample, block_count
):
    rank = factor_b.shape[0]
    devices = lax.axis_size("row")
    position = lax.axis_index("row")
    span = sample_k.shape[2]
    samples = sample_j.shape[0]
    tiles, slots, lanes = block_values.shape[2:]
    assert 2 * rank == LANES and lanes == LANES
    pairs = samples // 2
    f32 = jnp.float32
    c_base = jnp.full((1,), position * factor_c.shape[1], jnp.int32)
    b_base = jnp.full((1,), position * factor_b.shape[1], jnp.int32)
    c_out = pl.pallas_call(
        functools.partial(outgoing_kernel, span=span),
        out_shape=shape((pairs, LANES), jnp.bfloat16),
        in_specs=[SMEM, SMEM, VMEM],
        out_specs=VMEM,
        scratch_shapes=[
            pltpu.VMEM((factor_c.shape[1], LANES), f32),
            pltpu.VMEM((pairs, LANES), f32),
        ],
        name="outgoing",
    )(c_base, sample_k.reshape(-1), factor_c)
    c_in = lax.all_to_all(
        c_out.reshape(devices, pairs // devices, LANES), "row", split_axis=0, concat_axis=0, tiled=True
    ).reshape(pairs, LANES)
    weighted_b = pl.pallas_call(
        functools.partial(weighted_b_kernel, span=span),
        out_shape=shape((pairs, LANES), f32),
        in_specs=[SMEM, SMEM, VMEM, VMEM],
        out_specs=VMEM,
        scratch_shapes=[pltpu.VMEM((factor_b.shape[1], LANES), f32)],
        name="weighted_b",
    )(b_base, sample_j, sample_weight.reshape(2 * devices, span // 2), factor_b)
    blocks = tiles * slots
    payload = pl.pallas_call(
        functools.partial(sketch_kernel, span=span),
        out_shape=shape((devices, 2 * blocks + rank // 2, LANES), f32),
        in_specs=[SMEM, SMEM, SMEM, VMEM, VMEM, VMEM],
        out_specs=VMEM,
        scratch_shapes=[
            pltpu.VMEM((pairs, LANES), f32),
            pltpu.VMEM((devices * blocks, LANES), f32),
        ],
        name="sketch",
    )(
        block_sample.reshape(-1),
        block_count.reshape(-1),
        sample_weight,
        weighted_b,
        c_in,
        block_values.reshape(devices * blocks, LANES),
    )
    received = lax.all_to_all(payload, "row", split_axis=0, concat_axis=0, tiled=True)
    total_rows = tiles * LANES * devices
    update, sums = pl.pallas_call(
        functools.partial(
            solve_kernel,
            tiles=tiles,
            slots=slots,
            total_rows=total_rows,
            total_samples=samples * devices,
        ),
        out_shape=(shape((rank, tiles * LANES), f32), shape((devices, 8, LANES), f32)),
        in_specs=[VMEM],
        out_specs=(VMEM, VMEM),
        name="solve",
    )(received)
    all_sums = lax.all_to_all(sums, "row", split_axis=0, concat_axis=0, tiled=True)
    factor_new, scales = pl.pallas_call(
        functools.partial(scale_kernel, total_rows=total_rows),
        out_shape=(shape((rank, tiles * LANES), jnp.bfloat16), shape((8, LANES), f32)),
        in_specs=[VMEM, VMEM],
        out_specs=(VMEM, VMEM),
        name="scale",
    )(all_sums, update)
    return factor_new, scales[0, :rank]


def solution(mesh):
    in_specs = (
        P(None, ("groups", "row")),
        P(None, ("groups", "row")),
        P(("groups", "row")),
        P(None, ("groups", "row"), None),
        P(("groups", "row")),
        P(("groups", "row"), None, None, None, None),
        P(("groups", "row"), None, None, None),
        P(("groups", "row"), None, None, None),
    )
    out_specs = (P(None, ("groups", "row")), P("groups"))
    return jax.shard_map(shards, mesh=mesh, in_specs=in_specs, out_specs=out_specs, check_vma=False)
```

```python
import functools

import jax
import jax.numpy as jnp
from jax import lax
from jax.experimental import pallas as pl
from jax.experimental.pallas import tpu as pltpu
from jax.sharding import PartitionSpec as P

LANES = 128
HIGHEST = lax.Precision.HIGHEST
VMEM = pl.BlockSpec(memory_space=pltpu.VMEM)
SMEM = pl.BlockSpec(memory_space=pltpu.SMEM)
OVER_ROWS = (((0,), (0,)), ((), ()))


def lane_index(shape):
    return lax.broadcasted_iota(jnp.int32, shape, 1)


def fill_table(factor_ref, table_ref):
    columns = factor_ref.shape[1]

    def step(chunk, carry):
        start = pl.multiple_of(chunk * LANES, LANES)
        block = factor_ref[:, pl.ds(start, LANES)].astype(jnp.float32)
        table_ref[pl.ds(start, LANES), :] = jnp.concatenate([block, block], axis=0).T
        return carry

    lax.fori_loop(0, columns // LANES, step, 0)


def start_indices(base_ref, index_ref, local_ref, scalar_ref, sem):
    local_ref[...] = index_ref[...] - base_ref[0]
    copy = pltpu.make_async_copy(local_ref, scalar_ref, sem)
    copy.start()
    return copy


def gather_pairs(scalar_ref, table_ref, rows_ref, span):
    half = span // 2
    step_rows = min(LANES, half)
    low = lane_index((1, LANES)) < LANES // 2

    def step(q, carry):
        row = pl.multiple_of(q * step_rows, step_rows)
        first = row + lax.div(row, half) * half
        index_row = lax.div(first, LANES)
        for u in range(step_rows):
            ahead, column = divmod(u + half, LANES)
            a = scalar_ref[index_row, u]
            b = scalar_ref[index_row + ahead, column]
            rows_ref[pl.ds(row + u, 1), :] = jnp.where(
                low, table_ref[pl.ds(a, 1), :], table_ref[pl.ds(b, 1), :]
            )
        return carry

    lax.fori_loop(0, rows_ref.shape[0] // step_rows, step, 0)


def outgoing_kernel(
    base_ref, index_ref, factor_ref, out_ref, table_ref, rows_ref, local_ref, scalar_ref, sem, *, span
):
    copy = start_indices(base_ref, index_ref, local_ref, scalar_ref, sem)
    fill_table(factor_ref, table_ref)
    copy.wait()
    gather_pairs(scalar_ref, table_ref, rows_ref, span)
    out_ref[...] = rows_ref[...].astype(jnp.bfloat16)


def weighted_b_kernel(
    base_ref, count_ref, index_ref, weight_ref, factor_ref, values_ref,
    out_ref, masked_ref, table_ref, local_ref, scalar_ref, sem, *, span
):
    half = span // 2
    copy = start_indices(base_ref, index_ref, local_ref, scalar_ref, sem)
    fill_table(factor_ref, table_ref)
    copy.wait()
    gather_pairs(scalar_ref, table_ref, out_ref, span)
    turned = weight_ref[...].T
    low = lane_index((half, LANES)) < LANES // 2
    for e in range(out_ref.shape[0] // half):
        weights = jnp.where(low, turned[:, 2 * e : 2 * e + 1], turned[:, 2 * e + 1 : 2 * e + 2])
        out_ref[e * half : (e + 1) * half, :] = out_ref[e * half : (e + 1) * half, :] * weights
    masked_ref[...] = values_ref[...].astype(jnp.float32)
    lane = lane_index((1, LANES))
    step_rows = 16

    def mask_step(q, carry):
        row = pl.multiple_of(q * step_rows, step_rows)
        for u in range(step_rows):
            value_row = masked_ref[pl.ds(row + u, 1), :]
            masked_ref[pl.ds(row + u, 1), :] = jnp.where(lane < count_ref[row + u], value_row, 0.0)
        return carry

    lax.fori_loop(0, values_ref.shape[0] // step_rows, mask_step, 0)


def sketch_kernel(
    sample_ref, count_ref, weight_ref, wb_ref, c_ref, values_ref, out_ref, sketch_ref, *, span
):
    half = span // 2
    total_rows = wb_ref.shape[0]
    devices, _, _ = out_ref.shape
    blocks = values_ref.shape[0] // devices
    chunk = min(512, total_rows)

    def gram_step(q, acc):
        start = pl.multiple_of(q * chunk, chunk)
        x = wb_ref[pl.ds(start, chunk), :] * c_ref[pl.ds(start, chunk), :].astype(jnp.float32)
        sketch_ref[pl.ds(start, chunk), :] = x
        high = x.astype(jnp.bfloat16)
        rest = (x - high.astype(jnp.float32)).astype(jnp.bfloat16)
        both = jnp.concatenate([high, rest], axis=1)
        return acc + lax.dot_general(high, both, OVER_ROWS, preferred_element_type=jnp.float32)

    acc = lax.fori_loop(
        0, total_rows // chunk, gram_step, jnp.zeros((LANES, 2 * LANES), jnp.float32)
    )
    rank = LANES // 2
    cross = acc[:, LANES:]
    full = acc[:, :LANES] + cross + cross.T
    gram = full[:rank] + pltpu.roll(full[rank:], rank, 1)
    low = lane_index((1, LANES)) < rank
    packed = jnp.where(low, gram[: rank // 2], pltpu.roll(gram[rank // 2 :], rank, 1))

    def count_step(q, total):
        for u in range(blocks):
            total = total + count_ref[q * blocks + u]
        return total

    live = lax.fori_loop(0, devices, count_step, jnp.int32(0)).astype(jnp.float32)

    def pick_step(q, carry):
        for u in range(blocks):
            j = q * blocks + u
            s = sample_ref[j]
            e = lax.div(s, span)
            i = s - e * span
            upper = i >= half
            row = e * half + jnp.where(upper, i - half, i)
            scaled = sketch_ref[pl.ds(row, 1), :] * weight_ref[s]
            picked = jnp.where(upper, pltpu.roll(scaled, rank, 1), scaled)
            rounded = picked.astype(jnp.bfloat16).astype(jnp.float32)
            out_ref[q, blocks + u : blocks + u + 1, :] = jnp.where(low, rounded, live)
        out_ref[q, :blocks, :] = values_ref[pl.ds(pl.multiple_of(q * blocks, blocks), blocks), :]
        out_ref[q, 2 * blocks :, :] = packed
        return carry

    lax.fori_loop(0, devices, pick_step, 0)


def solve_kernel(in_ref, update_ref, sums_ref, *, tiles, slots, total_rows, total_samples):
    devices = in_ref.shape[0]
    rank = LANES // 2
    blocks = tiles * slots
    summed = in_ref[0, 2 * blocks :, :]
    live_row = in_ref[0, blocks : blocks + 1, :]
    for p in range(1, devices):
        summed = summed + in_ref[p, 2 * blocks :, :]
        live_row = live_row + in_ref[p, blocks : blocks + 1, :]
    gram = jnp.concatenate([summed, pltpu.roll(summed, rank, 1)], axis=0)
    ridge = 0.05 * pltpu.roll(live_row, rank, 1)[:, 0:1] / total_rows
    lane = lane_index((rank, LANES))
    sub = lax.broadcasted_iota(jnp.int32, (rank, LANES), 0)
    state = gram / total_samples + jnp.where(lane == sub, ridge, 0.0)
    lane_row = lane_index((1, LANES))
    for k in range(rank):
        pivot = 1.0 / state[k : k + 1, k : k + 1]
        row = jnp.where(lane_row == k, 1.0, state[k : k + 1, :]) * pivot
        column = state[:, k : k + 1]
        rest = jnp.where(lane == k, 0.0, state)
        state = jnp.where(sub == k, row, rest - column * row)
    inverse = state[:, :rank]
    values = in_ref[:, :blocks, :].reshape(devices * blocks, LANES).astype(jnp.bfloat16)
    rows = in_ref[:, blocks : 2 * blocks, :].reshape(devices * blocks, LANES)
    wide = lane_index(rows.shape)
    doubled = jnp.where(wide < rank, rows, pltpu.roll(rows, rank, 1))
    tile_of = lax.div(
        lax.rem(lax.broadcasted_iota(jnp.int32, rows.shape, 0), blocks), slots
    )
    parts = []
    for g in range(0, tiles, 2):
        wanted = jnp.where(wide < rank, g, g + 1)
        left = jnp.where(tile_of == wanted, doubled, 0.0).astype(jnp.bfloat16)
        both = lax.dot_general(left, values, OVER_ROWS, preferred_element_type=jnp.float32)
        parts += [both[:rank], both[rank:]]
    gathered = jnp.concatenate(parts[:tiles], axis=1)
    update = jnp.dot(inverse, gathered, precision=HIGHEST, preferred_element_type=jnp.float32)
    update_ref[...] = update
    column_sums = jnp.sum(update * update, axis=1, keepdims=True)
    turned = jnp.broadcast_to(
        jnp.concatenate([column_sums, column_sums], axis=0), (LANES, LANES)
    ).T
    for p in range(devices):
        sums_ref[p] = turned[:8]


def scale_kernel(sums_ref, update_ref, out_ref, scales_ref, *, total_rows):
    rank = update_ref.shape[0]
    summed = sums_ref[0]
    for p in range(1, sums_ref.shape[0]):
        summed = summed + sums_ref[p]
    scales = jnp.sqrt(summed / total_rows + 1e-06)
    scales_ref[...] = scales[0:1, :rank]
    column = jnp.broadcast_to(scales[0:1], (LANES, LANES)).T[:rank, 0:1]
    out_ref[...] = (update_ref[...] / column).astype(jnp.bfloat16)


def shape(dims, dtype):
    return jax.ShapeDtypeStruct(dims, dtype)


def shards(
    factor_b, factor_c, sample_j, sample_k, sample_weight, block_values, block_sample, block_count
):
    rank = factor_b.shape[0]
    devices = lax.axis_size("row")
    position = lax.axis_index("row")
    span = sample_k.shape[2]
    samples = sample_j.shape[0]
    tiles, slots, lanes = block_values.shape[2:]
    assert 2 * rank == LANES and lanes == LANES
    pairs = samples // 2
    f32 = jnp.float32
    c_base = jnp.full((1,), position * factor_c.shape[1], jnp.int32)
    b_base = jnp.full((1,), position * factor_b.shape[1], jnp.int32)
    index_shape = (samples // LANES, LANES)
    index_scratch = [
        pltpu.VMEM(index_shape, jnp.int32),
        pltpu.SMEM(index_shape, jnp.int32),
        pltpu.SemaphoreType.DMA,
    ]
    blocks = tiles * slots
    counts = block_count.reshape(-1)
    c_out = pl.pallas_call(
        functools.partial(outgoing_kernel, span=span),
        out_shape=shape((pairs, LANES), jnp.bfloat16),
        in_specs=[SMEM, VMEM, VMEM],
        out_specs=VMEM,
        scratch_shapes=[
            pltpu.VMEM((factor_c.shape[1], LANES), f32),
            pltpu.VMEM((pairs, LANES), f32),
            *index_scratch,
        ],
        name="outgoing",
    )(c_base, sample_k.reshape(index_shape), factor_c)
    c_in = lax.all_to_all(
        c_out.reshape(devices, pairs // devices, LANES), "row", split_axis=0, concat_axis=0, tiled=True
    ).reshape(pairs, LANES)
    weighted_b, masked = pl.pallas_call(
        functools.partial(weighted_b_kernel, span=span),
        out_shape=(shape((pairs, LANES), f32), shape((devices * blocks, LANES), f32)),
        in_specs=[SMEM, SMEM, VMEM, VMEM, VMEM, VMEM],
        out_specs=(VMEM, VMEM),
        scratch_shapes=[pltpu.VMEM((factor_b.shape[1], LANES), f32), *index_scratch],
        name="weighted_b",
    )(
        b_base,
        counts,
        sample_j.reshape(index_shape),
        sample_weight.reshape(2 * devices, span // 2),
        factor_b,
        block_values.reshape(devices * blocks, LANES),
    )
    payload = pl.pallas_call(
        functools.partial(sketch_kernel, span=span),
        out_shape=shape((devices, 2 * blocks + rank // 2, LANES), f32),
        in_specs=[SMEM, SMEM, SMEM, VMEM, VMEM, VMEM],
        out_specs=VMEM,
        scratch_shapes=[pltpu.VMEM((pairs, LANES), f32)],
        name="sketch",
    )(block_sample.reshape(-1), counts, sample_weight, weighted_b, c_in, masked)
    received = lax.all_to_all(payload, "row", split_axis=0, concat_axis=0, tiled=True)
    total_rows = tiles * LANES * devices
    update, sums = pl.pallas_call(
        functools.partial(
            solve_kernel,
            tiles=tiles,
            slots=slots,
            total_rows=total_rows,
            total_samples=samples * devices,
        ),
        out_shape=(shape((rank, tiles * LANES), f32), shape((devices, 8, LANES), f32)),
        in_specs=[VMEM],
        out_specs=(VMEM, VMEM),
        name="solve",
    )(received)
    all_sums = lax.all_to_all(sums, "row", split_axis=0, concat_axis=0, tiled=True)
    factor_new, scales = pl.pallas_call(
        functools.partial(scale_kernel, total_rows=total_rows),
        out_shape=(shape((rank, tiles * LANES), jnp.bfloat16), shape((1, rank), f32)),
        in_specs=[VMEM, VMEM],
        out_specs=(VMEM, VMEM),
        name="scale",
    )(all_sums, update)
    return factor_new, scales.reshape(rank)


def solution(mesh):
    in_specs = (
        P(None, ("groups", "row")),
        P(None, ("groups", "row")),
        P(("groups", "row")),
        P(None, ("groups", "row"), None),
        P(("groups", "row")),
        P(("groups", "row"), None, None, None, None),
        P(("groups", "row"), None, None, None),
        P(("groups", "row"), None, None, None),
    )
    out_specs = (P(None, ("groups", "row")), P("groups"))
    return jax.shard_map(shards, mesh=mesh, in_specs=in_specs, out_specs=out_specs, check_vma=False)
```

```python
import functools

import jax
import jax.numpy as jnp
from jax import lax
from jax.experimental import pallas as pl
from jax.experimental.pallas import tpu as pltpu
from jax.sharding import PartitionSpec as P

LANES = 128
HIGHEST = lax.Precision.HIGHEST
VMEM = pl.BlockSpec(memory_space=pltpu.VMEM)
SMEM = pl.BlockSpec(memory_space=pltpu.SMEM)
OVER_ROWS = (((0,), (0,)), ((), ()))


def lane_index(shape):
    return lax.broadcasted_iota(jnp.int32, shape, 1)


def fill_table(factor_ref, table_ref):
    columns = factor_ref.shape[1]

    def step(chunk, carry):
        start = pl.multiple_of(chunk * LANES, LANES)
        block = factor_ref[:, pl.ds(start, LANES)].astype(jnp.float32)
        table_ref[pl.ds(start, LANES), :] = jnp.concatenate([block, block], axis=0).T
        return carry

    lax.fori_loop(0, columns // LANES, step, 0)


def start_indices(base_ref, index_ref, local_ref, scalar_ref, sem):
    local_ref[...] = index_ref[...] - base_ref[0]
    copy = pltpu.make_async_copy(local_ref, scalar_ref, sem)
    copy.start()
    return copy


def gather_pairs(scalar_ref, table_ref, rows_ref, span):
    half = span // 2
    step_rows = min(LANES, half)
    low = lane_index((1, LANES)) < LANES // 2

    def step(q, carry):
        row = pl.multiple_of(q * step_rows, step_rows)
        first = row + lax.div(row, half) * half
        index_row = lax.div(first, LANES)
        for u in range(step_rows):
            ahead, column = divmod(u + half, LANES)
            a = scalar_ref[index_row, u]
            b = scalar_ref[index_row + ahead, column]
            rows_ref[pl.ds(row + u, 1), :] = jnp.where(
                low, table_ref[pl.ds(a, 1), :], table_ref[pl.ds(b, 1), :]
            )
        return carry

    lax.fori_loop(0, rows_ref.shape[0] // step_rows, step, 0)


def outgoing_kernel(
    base_ref, index_ref, factor_ref, out_ref, table_ref, rows_ref, local_ref, scalar_ref, sem, *, span
):
    copy = start_indices(base_ref, index_ref, local_ref, scalar_ref, sem)
    fill_table(factor_ref, table_ref)
    copy.wait()
    gather_pairs(scalar_ref, table_ref, rows_ref, span)
    out_ref[...] = rows_ref[...].astype(jnp.bfloat16)


def weighted_b_kernel(
    base_ref, count_ref, index_ref, weight_ref, factor_ref, values_ref,
    out_ref, masked_ref, table_ref, local_ref, scalar_ref, sem, wide_ref, *, span
):
    half = span // 2
    copy = start_indices(base_ref, index_ref, local_ref, scalar_ref, sem)
    fill_table(factor_ref, table_ref)
    copy.wait()
    gather_pairs(scalar_ref, table_ref, out_ref, span)
    turned = weight_ref[...].T
    low = lane_index((half, LANES)) < LANES // 2
    for e in range(out_ref.shape[0] // half):
        weights = jnp.where(low, turned[:, 2 * e : 2 * e + 1], turned[:, 2 * e + 1 : 2 * e + 2])
        out_ref[e * half : (e + 1) * half, :] = out_ref[e * half : (e + 1) * half, :] * weights
    wide_ref[...] = values_ref[...].astype(jnp.float32)
    lane = lane_index((1, LANES))
    step_rows = 16

    def mask_step(q, carry):
        row = pl.multiple_of(q * step_rows, step_rows)
        for u in range(step_rows):
            value_row = wide_ref[pl.ds(row + u, 1), :]
            wide_ref[pl.ds(row + u, 1), :] = jnp.where(lane < count_ref[row + u], value_row, 0.0)
        return carry

    lax.fori_loop(0, values_ref.shape[0] // step_rows, mask_step, 0)
    masked_ref[...] = wide_ref[...].astype(jnp.bfloat16)


def split(x):
    high = x.astype(jnp.bfloat16).astype(jnp.float32)
    return high, x - high


def sketch_kernel(
    sample_ref, count_ref, weight_ref, wb_ref, c_ref, values_ref, out_ref, sketch_ref, picked_ref, *, span
):
    half = span // 2
    total_rows = wb_ref.shape[0]
    devices, _, _ = out_ref.shape
    blocks = values_ref.shape[0] // devices
    chunk = min(512, total_rows)

    def gram_step(q, acc):
        start = pl.multiple_of(q * chunk, chunk)
        x = wb_ref[pl.ds(start, chunk), :] * c_ref[pl.ds(start, chunk), :].astype(jnp.float32)
        sketch_ref[pl.ds(start, chunk), :] = x
        high = x.astype(jnp.bfloat16)
        rest = (x - high.astype(jnp.float32)).astype(jnp.bfloat16)
        both = jnp.concatenate([high, rest], axis=1)
        return acc + lax.dot_general(high, both, OVER_ROWS, preferred_element_type=jnp.float32)

    acc = lax.fori_loop(
        0, total_rows // chunk, gram_step, jnp.zeros((LANES, 2 * LANES), jnp.float32)
    )
    rank = LANES // 2
    cross = acc[:, LANES:]
    full = acc[:, :LANES] + cross + cross.T
    gram = full[:rank] + pltpu.roll(full[rank:], rank, 1)
    low = lane_index((1, LANES)) < rank
    quarter = rank // 2
    lane = lane_index((quarter, LANES))
    sub = lax.broadcasted_iota(jnp.int32, (quarter, LANES), 0)
    top, bottom = gram[:quarter], gram[quarter:]
    folded = jnp.where(lane < jnp.minimum(sub, quarter), pltpu.roll(bottom, LANES - quarter, 1), top)
    high, rest = split(folded)
    packed = jnp.where(low, high, pltpu.roll(rest, rank, 1)).astype(jnp.bfloat16)
    diagonal = jnp.sum(jnp.where(lane == sub + quarter, bottom, 0.0), axis=0, keepdims=True)
    high, rest = split(diagonal)
    third = lane_index((1, LANES)) < rank + quarter
    diagonal_row = jnp.where(third, pltpu.roll(high, quarter, 1), pltpu.roll(rest, rank, 1))

    def count_step(q, total):
        for u in range(blocks):
            total = total + count_ref[q * blocks + u]
        return total

    live = lax.fori_loop(0, devices, count_step, jnp.int32(0)).astype(jnp.float32)
    high, rest = split(jnp.full((1, LANES), live, jnp.float32))
    spare = [diagonal_row, jnp.where(third, high, rest)]

    def pick_step(q, carry):
        for u in range(blocks):
            j = q * blocks + u
            s = sample_ref[j]
            e = lax.div(s, span)
            i = s - e * span
            upper = i >= half
            row = e * half + jnp.where(upper, i - half, i)
            scaled = sketch_ref[pl.ds(row, 1), :] * weight_ref[s]
            picked = jnp.where(upper, pltpu.roll(scaled, rank, 1), scaled)
            picked_ref[q, u : u + 1, :] = jnp.where(low, picked, spare[u]) if u < 2 else picked
        out_ref[q, :blocks, :] = values_ref[pl.ds(pl.multiple_of(q * blocks, blocks), blocks), :]
        out_ref[q, blocks : 2 * blocks, :] = picked_ref[q].astype(jnp.bfloat16)
        out_ref[q, 2 * blocks :, :] = packed
        return carry

    lax.fori_loop(0, devices, pick_step, 0)


def solve_kernel(in_ref, update_ref, sums_ref, *, tiles, slots, total_rows, total_samples):
    devices = in_ref.shape[0]
    rank = LANES // 2
    blocks = tiles * slots
    f32 = jnp.float32
    summed = in_ref[0, 2 * blocks :, :].astype(f32)
    spare = in_ref[0, blocks : 2 * blocks, :].astype(f32)
    for p in range(1, devices):
        summed = summed + in_ref[p, 2 * blocks :, :].astype(f32)
        spare = spare + in_ref[p, blocks : 2 * blocks, :].astype(f32)
    quarter = rank // 2
    lane = lane_index((quarter, LANES))
    sub = lax.broadcasted_iota(jnp.int32, (quarter, LANES), 0)
    folded = summed + pltpu.roll(summed, rank, 1)
    joined = spare[0:8] + pltpu.roll(spare[0:8], LANES - quarter, 1)
    joined = pltpu.roll(joined, rank, 1)
    turned = jnp.concatenate([folded] + [jnp.zeros_like(folded)] * 3, axis=0).T
    mirror = turned[:quarter]
    first = jnp.where(lane < sub, mirror, folded)
    first = jnp.where(lane < quarter, first, folded)
    last = jnp.where(lane < sub, folded, jnp.where(lane > sub, mirror, joined[0:1]))
    last = jnp.where(lane < quarter, turned[quarter:rank], pltpu.roll(last, quarter, 1))
    gram = jnp.concatenate([first, last], axis=0)
    ridge = 0.05 * joined[1:2, 0:1] / total_rows
    lane = lane_index((rank, LANES))
    sub = lax.broadcasted_iota(jnp.int32, (rank, LANES), 0)
    state = gram / total_samples + jnp.where(lane == sub, ridge, 0.0)
    lane_row = lane_index((1, LANES))
    for k in range(rank):
        pivot = 1.0 / state[k : k + 1, k : k + 1]
        row = jnp.where(lane_row == k, 1.0, state[k : k + 1, :]) * pivot
        column = state[:, k : k + 1]
        rest = jnp.where(lane == k, 0.0, state)
        state = jnp.where(sub == k, row, rest - column * row)
    inverse = state[:, :rank]
    values = in_ref[:, :blocks, :].reshape(devices * blocks, LANES)
    rows = in_ref[:, blocks : 2 * blocks, :].reshape(devices * blocks, LANES).astype(f32)
    wide = lane_index(rows.shape)
    doubled = jnp.where(wide < rank, rows, pltpu.roll(rows, rank, 1))
    tile_of = lax.div(
        lax.rem(lax.broadcasted_iota(jnp.int32, rows.shape, 0), blocks), slots
    )
    parts = []
    for g in range(0, tiles, 2):
        wanted = jnp.where(wide < rank, g, g + 1)
        left = jnp.where(tile_of == wanted, doubled, 0.0).astype(jnp.bfloat16)
        both = lax.dot_general(left, values, OVER_ROWS, preferred_element_type=jnp.float32)
        parts += [both[:rank], both[rank:]]
    gathered = jnp.concatenate(parts[:tiles], axis=1)
    update = jnp.dot(inverse, gathered, precision=HIGHEST, preferred_element_type=jnp.float32)
    update_ref[...] = update
    column_sums = jnp.sum(update * update, axis=1, keepdims=True)
    turned = jnp.broadcast_to(
        jnp.concatenate([column_sums, column_sums], axis=0), (LANES, LANES)
    ).T
    for p in range(devices):
        sums_ref[p] = turned[:8]


def scale_kernel(sums_ref, update_ref, out_ref, scales_ref, *, total_rows):
    rank = update_ref.shape[0]
    summed = sums_ref[0]
    for p in range(1, sums_ref.shape[0]):
        summed = summed + sums_ref[p]
    scales = jnp.sqrt(summed / total_rows + 1e-06)
    scales_ref[...] = scales[0:1, :rank]
    column = jnp.broadcast_to(scales[0:1], (LANES, LANES)).T[:rank, 0:1]
    out_ref[...] = (update_ref[...] / column).astype(jnp.bfloat16)


def shape(dims, dtype):
    return jax.ShapeDtypeStruct(dims, dtype)


def shards(
    factor_b, factor_c, sample_j, sample_k, sample_weight, block_values, block_sample, block_count
):
    rank = factor_b.shape[0]
    devices = lax.axis_size("row")
    position = lax.axis_index("row")
    span = sample_k.shape[2]
    samples = sample_j.shape[0]
    tiles, slots, lanes = block_values.shape[2:]
    assert 2 * rank == LANES and lanes == LANES
    pairs = samples // 2
    f32 = jnp.float32
    c_base = jnp.full((1,), position * factor_c.shape[1], jnp.int32)
    b_base = jnp.full((1,), position * factor_b.shape[1], jnp.int32)
    index_shape = (samples // LANES, LANES)
    index_scratch = [
        pltpu.VMEM(index_shape, jnp.int32),
        pltpu.SMEM(index_shape, jnp.int32),
        pltpu.SemaphoreType.DMA,
    ]
    blocks = tiles * slots
    counts = block_count.reshape(-1)
    c_out = pl.pallas_call(
        functools.partial(outgoing_kernel, span=span),
        out_shape=shape((pairs, LANES), jnp.bfloat16),
        in_specs=[SMEM, VMEM, VMEM],
        out_specs=VMEM,
        scratch_shapes=[
            pltpu.VMEM((factor_c.shape[1], LANES), f32),
            pltpu.VMEM((pairs, LANES), f32),
            *index_scratch,
        ],
        name="outgoing",
    )(c_base, sample_k.reshape(index_shape), factor_c)
    c_in = lax.all_to_all(
        c_out.reshape(devices, pairs // devices, LANES), "row", split_axis=0, concat_axis=0, tiled=True
    ).reshape(pairs, LANES)
    weighted_b, masked = pl.pallas_call(
        functools.partial(weighted_b_kernel, span=span),
        out_shape=(shape((pairs, LANES), f32), shape((devices * blocks, LANES), jnp.bfloat16)),
        in_specs=[SMEM, SMEM, VMEM, VMEM, VMEM, VMEM],
        out_specs=(VMEM, VMEM),
        scratch_shapes=[
            pltpu.VMEM((factor_b.shape[1], LANES), f32),
            *index_scratch,
            pltpu.VMEM((devices * blocks, LANES), f32),
        ],
        name="weighted_b",
    )(
        b_base,
        counts,
        sample_j.reshape(index_shape),
        sample_weight.reshape(2 * devices, span // 2),
        factor_b,
        block_values.reshape(devices * blocks, LANES),
    )
    payload = pl.pallas_call(
        functools.partial(sketch_kernel, span=span),
        out_shape=shape((devices, 2 * blocks + rank // 2, LANES), jnp.bfloat16),
        in_specs=[SMEM, SMEM, SMEM, VMEM, VMEM, VMEM],
        out_specs=VMEM,
        scratch_shapes=[
            pltpu.VMEM((pairs, LANES), f32),
            pltpu.VMEM((devices, blocks, LANES), f32),
        ],
        name="sketch",
    )(block_sample.reshape(-1), counts, sample_weight, weighted_b, c_in, masked)
    received = lax.all_to_all(payload, "row", split_axis=0, concat_axis=0, tiled=True)
    total_rows = tiles * LANES * devices
    update, sums = pl.pallas_call(
        functools.partial(
            solve_kernel,
            tiles=tiles,
            slots=slots,
            total_rows=total_rows,
            total_samples=samples * devices,
        ),
        out_shape=(shape((rank, tiles * LANES), f32), shape((devices, 8, LANES), f32)),
        in_specs=[VMEM],
        out_specs=(VMEM, VMEM),
        name="solve",
    )(received)
    all_sums = lax.all_to_all(sums, "row", split_axis=0, concat_axis=0, tiled=True)
    factor_new, scales = pl.pallas_call(
        functools.partial(scale_kernel, total_rows=total_rows),
        out_shape=(shape((rank, tiles * LANES), jnp.bfloat16), shape((1, rank), f32)),
        in_specs=[VMEM, VMEM],
        out_specs=(VMEM, VMEM),
        name="scale",
    )(all_sums, update)
    return factor_new, scales.reshape(rank)


def solution(mesh):
    in_specs = (
        P(None, ("groups", "row")),
        P(None, ("groups", "row")),
        P(("groups", "row")),
        P(None, ("groups", "row"), None),
        P(("groups", "row")),
        P(("groups", "row"), None, None, None, None),
        P(("groups", "row"), None, None, None),
        P(("groups", "row"), None, None, None),
    )
    out_specs = (P(None, ("groups", "row")), P("groups"))
    return jax.shard_map(shards, mesh=mesh, in_specs=in_specs, out_specs=out_specs, check_vma=False)
```

```python
import functools

import jax
import jax.numpy as jnp
from jax import lax
from jax.experimental import pallas as pl
from jax.experimental.pallas import tpu as pltpu
from jax.sharding import PartitionSpec as P

LANES = 128
HIGHEST = lax.Precision.HIGHEST
VMEM = pl.BlockSpec(memory_space=pltpu.VMEM)
SMEM = pl.BlockSpec(memory_space=pltpu.SMEM)
OVER_ROWS = (((0,), (0,)), ((), ()))


def lane_index(shape):
    return lax.broadcasted_iota(jnp.int32, shape, 1)


def fill_table(factor_ref, table_ref):
    columns = factor_ref.shape[1]

    def step(chunk, carry):
        start = pl.multiple_of(chunk * LANES, LANES)
        block = factor_ref[:, pl.ds(start, LANES)].astype(jnp.float32)
        table_ref[pl.ds(start, LANES), :] = jnp.concatenate([block, block], axis=0).T
        return carry

    lax.fori_loop(0, columns // LANES, step, 0)


def start_indices(base_ref, index_ref, local_ref, scalar_ref, sem):
    local_ref[...] = index_ref[...] - base_ref[0]
    copy = pltpu.make_async_copy(local_ref, scalar_ref, sem)
    copy.start()
    return copy


def gather_pairs(scalar_ref, table_ref, rows_ref, span):
    half = span // 2
    step_rows = min(LANES, half)
    low = lane_index((1, LANES)) < LANES // 2

    def step(q, carry):
        row = pl.multiple_of(q * step_rows, step_rows)
        first = row + lax.div(row, half) * half
        index_row = lax.div(first, LANES)
        for u in range(step_rows):
            ahead, column = divmod(u + half, LANES)
            a = scalar_ref[index_row, u]
            b = scalar_ref[index_row + ahead, column]
            rows_ref[pl.ds(row + u, 1), :] = jnp.where(
                low, table_ref[pl.ds(a, 1), :], table_ref[pl.ds(b, 1), :]
            )
        return carry

    lax.fori_loop(0, rows_ref.shape[0] // step_rows, step, 0)


def outgoing_kernel(
    base_ref, index_ref, factor_ref, out_ref, table_ref, rows_ref, local_ref, scalar_ref, sem, *, span
):
    copy = start_indices(base_ref, index_ref, local_ref, scalar_ref, sem)
    fill_table(factor_ref, table_ref)
    copy.wait()
    gather_pairs(scalar_ref, table_ref, rows_ref, span)
    out_ref[...] = rows_ref[...].astype(jnp.bfloat16)


def weighted_b_kernel(
    base_ref, count_ref, index_ref, weight_ref, factor_ref, values_ref,
    out_ref, masked_ref, table_ref, local_ref, scalar_ref, sem, wide_ref, *, span
):
    half = span // 2
    copy = start_indices(base_ref, index_ref, local_ref, scalar_ref, sem)
    fill_table(factor_ref, table_ref)
    copy.wait()
    gather_pairs(scalar_ref, table_ref, out_ref, span)
    turned = weight_ref[...].T
    low = lane_index((half, LANES)) < LANES // 2
    for e in range(out_ref.shape[0] // half):
        weights = jnp.where(low, turned[:, 2 * e : 2 * e + 1], turned[:, 2 * e + 1 : 2 * e + 2])
        out_ref[e * half : (e + 1) * half, :] = out_ref[e * half : (e + 1) * half, :] * weights
    wide_ref[...] = values_ref[...].astype(jnp.float32)
    lane = lane_index((1, LANES))
    step_rows = 16

    def mask_step(q, carry):
        row = pl.multiple_of(q * step_rows, step_rows)
        for u in range(step_rows):
            value_row = wide_ref[pl.ds(row + u, 1), :]
            wide_ref[pl.ds(row + u, 1), :] = jnp.where(lane < count_ref[row + u], value_row, 0.0)
        return carry

    lax.fori_loop(0, values_ref.shape[0] // step_rows, mask_step, 0)
    masked_ref[...] = wide_ref[...].astype(jnp.bfloat16)


def split(x):
    high = x.astype(jnp.bfloat16).astype(jnp.float32)
    return high, x - high


def sketch_kernel(
    sample_ref, count_ref, weight_ref, wb_ref, c_ref, values_ref, out_ref, sketch_ref, picked_ref, *, span
):
    half = span // 2
    total_rows = wb_ref.shape[0]
    devices, _, _ = out_ref.shape
    blocks = values_ref.shape[0] // devices
    chunk = min(512, total_rows)

    def gram_step(q, acc):
        start = pl.multiple_of(q * chunk, chunk)
        x = wb_ref[pl.ds(start, chunk), :] * c_ref[pl.ds(start, chunk), :].astype(jnp.float32)
        sketch_ref[pl.ds(start, chunk), :] = x
        high = x.astype(jnp.bfloat16)
        rest = (x - high.astype(jnp.float32)).astype(jnp.bfloat16)
        both = jnp.concatenate([high, rest], axis=1)
        return acc + lax.dot_general(high, both, OVER_ROWS, preferred_element_type=jnp.float32)

    acc = lax.fori_loop(
        0, total_rows // chunk, gram_step, jnp.zeros((LANES, 2 * LANES), jnp.float32)
    )
    rank = LANES // 2
    cross = acc[:, LANES:]
    full = acc[:, :LANES] + cross + cross.T
    gram = full[:rank] + pltpu.roll(full[rank:], rank, 1)
    low = lane_index((1, LANES)) < rank
    quarter = rank // 2
    lane = lane_index((quarter, LANES))
    sub = lax.broadcasted_iota(jnp.int32, (quarter, LANES), 0)
    top, bottom = gram[:quarter], gram[quarter:]
    folded = jnp.where(lane < jnp.minimum(sub, quarter), pltpu.roll(bottom, LANES - quarter, 1), top)
    high, rest = split(folded)
    packed = jnp.where(low, high, pltpu.roll(rest, rank, 1)).astype(jnp.bfloat16)
    diagonal = jnp.sum(jnp.where(lane == sub + quarter, bottom, 0.0), axis=0, keepdims=True)
    high, rest = split(diagonal)
    third = lane_index((1, LANES)) < rank + quarter
    diagonal_row = jnp.where(third, pltpu.roll(high, quarter, 1), pltpu.roll(rest, rank, 1))

    def count_step(q, total):
        for u in range(blocks):
            total = total + count_ref[q * blocks + u]
        return total

    live = lax.fori_loop(0, devices, count_step, jnp.int32(0)).astype(jnp.float32)
    high, rest = split(jnp.full((1, LANES), live, jnp.float32))
    spare = [diagonal_row, jnp.where(third, high, rest)]

    def pick_step(q, carry):
        for u in range(blocks):
            j = q * blocks + u
            s = sample_ref[j]
            e = lax.div(s, span)
            i = s - e * span
            upper = i >= half
            row = e * half + jnp.where(upper, i - half, i)
            scaled = sketch_ref[pl.ds(row, 1), :] * weight_ref[s]
            picked = jnp.where(upper, pltpu.roll(scaled, rank, 1), scaled)
            picked_ref[q, u : u + 1, :] = jnp.where(low, picked, spare[u]) if u < 2 else picked
        out_ref[q, :blocks, :] = values_ref[pl.ds(pl.multiple_of(q * blocks, blocks), blocks), :]
        out_ref[q, blocks : 2 * blocks, :] = picked_ref[q].astype(jnp.bfloat16)
        out_ref[q, 2 * blocks :, :] = packed
        return carry

    lax.fori_loop(0, devices, pick_step, 0)


def solve_kernel(in_ref, update_ref, sums_ref, *, tiles, slots, total_rows, total_samples):
    devices = in_ref.shape[0]
    rank = LANES // 2
    blocks = tiles * slots
    f32 = jnp.float32
    summed = in_ref[0, 2 * blocks :, :].astype(f32)
    spare = in_ref[0, blocks : 2 * blocks, :].astype(f32)
    for p in range(1, devices):
        summed = summed + in_ref[p, 2 * blocks :, :].astype(f32)
        spare = spare + in_ref[p, blocks : 2 * blocks, :].astype(f32)
    quarter = rank // 2
    lane = lane_index((quarter, LANES))
    sub = lax.broadcasted_iota(jnp.int32, (quarter, LANES), 0)
    folded = summed + pltpu.roll(summed, rank, 1)
    joined = spare[0:8] + pltpu.roll(spare[0:8], LANES - quarter, 1)
    joined = pltpu.roll(joined, rank, 1)
    turned = jnp.concatenate([folded] + [jnp.zeros_like(folded)] * 3, axis=0).T
    mirror = turned[:quarter]
    first = jnp.where(lane < sub, mirror, folded)
    first = jnp.where(lane < quarter, first, folded)
    last = jnp.where(lane < sub, folded, jnp.where(lane > sub, mirror, joined[0:1]))
    last = jnp.where(lane < quarter, turned[quarter:rank], pltpu.roll(last, quarter, 1))
    gram = jnp.concatenate([first, last], axis=0)
    ridge = 0.05 * joined[1:2, 0:1] / total_rows
    lane = lane_index((rank, LANES))
    sub = lax.broadcasted_iota(jnp.int32, (rank, LANES), 0)
    state = gram / total_samples + jnp.where(lane == sub, ridge, 0.0)
    lane_row = lane_index((1, LANES))
    for k in range(0, rank, 2):
        upper, lower = state[k : k + 1, :], state[k + 1 : k + 2, :]
        p, q, r = upper[:, k : k + 1], upper[:, k + 1 : k + 2], lower[:, k + 1 : k + 2]
        scale = 1.0 / (p * r - q * q)
        here, after = lane_row == k, lane_row == k + 1
        upper = jnp.where(here, 1.0, jnp.where(after, 0.0, upper))
        lower = jnp.where(here, 0.0, jnp.where(after, 1.0, lower))
        first = (r * upper - q * lower) * scale
        last = (p * lower - q * upper) * scale
        rest = jnp.where((lane == k) | (lane == k + 1), 0.0, state)
        rest = rest - state[:, k : k + 1] * first - state[:, k + 1 : k + 2] * last
        state = jnp.where(sub == k, first, jnp.where(sub == k + 1, last, rest))
    inverse = state[:, :rank]
    values = in_ref[:, :blocks, :].reshape(devices * blocks, LANES)
    rows = in_ref[:, blocks : 2 * blocks, :].reshape(devices * blocks, LANES).astype(f32)
    wide = lane_index(rows.shape)
    doubled = jnp.where(wide < rank, rows, pltpu.roll(rows, rank, 1))
    tile_of = lax.div(
        lax.rem(lax.broadcasted_iota(jnp.int32, rows.shape, 0), blocks), slots
    )
    parts = []
    for g in range(0, tiles, 2):
        wanted = jnp.where(wide < rank, g, g + 1)
        left = jnp.where(tile_of == wanted, doubled, 0.0).astype(jnp.bfloat16)
        both = lax.dot_general(left, values, OVER_ROWS, preferred_element_type=jnp.float32)
        parts += [both[:rank], both[rank:]]
    gathered = jnp.concatenate(parts[:tiles], axis=1)
    update = jnp.dot(inverse, gathered, precision=HIGHEST, preferred_element_type=jnp.float32)
    update_ref[...] = update
    column_sums = jnp.sum(update * update, axis=1, keepdims=True)
    turned = jnp.broadcast_to(
        jnp.concatenate([column_sums, column_sums], axis=0), (LANES, LANES)
    ).T
    for p in range(devices):
        sums_ref[p] = turned[:8]


def scale_kernel(sums_ref, update_ref, out_ref, scales_ref, *, total_rows):
    rank = update_ref.shape[0]
    summed = sums_ref[0]
    for p in range(1, sums_ref.shape[0]):
        summed = summed + sums_ref[p]
    scales = jnp.sqrt(summed / total_rows + 1e-06)
    scales_ref[...] = scales[0:1, :rank]
    column = jnp.broadcast_to(scales[0:1], (LANES, LANES)).T[:rank, 0:1]
    out_ref[...] = (update_ref[...] / column).astype(jnp.bfloat16)


def shape(dims, dtype):
    return jax.ShapeDtypeStruct(dims, dtype)


def shards(
    factor_b, factor_c, sample_j, sample_k, sample_weight, block_values, block_sample, block_count
):
    rank = factor_b.shape[0]
    devices = lax.axis_size("row")
    position = lax.axis_index("row")
    span = sample_k.shape[2]
    samples = sample_j.shape[0]
    tiles, slots, lanes = block_values.shape[2:]
    assert 2 * rank == LANES and lanes == LANES
    pairs = samples // 2
    f32 = jnp.float32
    c_base = jnp.full((1,), position * factor_c.shape[1], jnp.int32)
    b_base = jnp.full((1,), position * factor_b.shape[1], jnp.int32)
    index_shape = (samples // LANES, LANES)
    index_scratch = [
        pltpu.VMEM(index_shape, jnp.int32),
        pltpu.SMEM(index_shape, jnp.int32),
        pltpu.SemaphoreType.DMA,
    ]
    blocks = tiles * slots
    counts = block_count.reshape(-1)
    c_out = pl.pallas_call(
        functools.partial(outgoing_kernel, span=span),
        out_shape=shape((pairs, LANES), jnp.bfloat16),
        in_specs=[SMEM, VMEM, VMEM],
        out_specs=VMEM,
        scratch_shapes=[
            pltpu.VMEM((factor_c.shape[1], LANES), f32),
            pltpu.VMEM((pairs, LANES), f32),
            *index_scratch,
        ],
        name="outgoing",
    )(c_base, sample_k.reshape(index_shape), factor_c)
    c_in = lax.all_to_all(
        c_out.reshape(devices, pairs // devices, LANES), "row", split_axis=0, concat_axis=0, tiled=True
    ).reshape(pairs, LANES)
    weighted_b, masked = pl.pallas_call(
        functools.partial(weighted_b_kernel, span=span),
        out_shape=(shape((pairs, LANES), f32), shape((devices * blocks, LANES), jnp.bfloat16)),
        in_specs=[SMEM, SMEM, VMEM, VMEM, VMEM, VMEM],
        out_specs=(VMEM, VMEM),
        scratch_shapes=[
            pltpu.VMEM((factor_b.shape[1], LANES), f32),
            *index_scratch,
            pltpu.VMEM((devices * blocks, LANES), f32),
        ],
        name="weighted_b",
    )(
        b_base,
        counts,
        sample_j.reshape(index_shape),
        sample_weight.reshape(2 * devices, span // 2),
        factor_b,
        block_values.reshape(devices * blocks, LANES),
    )
    payload = pl.pallas_call(
        functools.partial(sketch_kernel, span=span),
        out_shape=shape((devices, 2 * blocks + rank // 2, LANES), jnp.bfloat16),
        in_specs=[SMEM, SMEM, SMEM, VMEM, VMEM, VMEM],
        out_specs=VMEM,
        scratch_shapes=[
            pltpu.VMEM((pairs, LANES), f32),
            pltpu.VMEM((devices, blocks, LANES), f32),
        ],
        name="sketch",
    )(block_sample.reshape(-1), counts, sample_weight, weighted_b, c_in, masked)
    received = lax.all_to_all(payload, "row", split_axis=0, concat_axis=0, tiled=True)
    total_rows = tiles * LANES * devices
    update, sums = pl.pallas_call(
        functools.partial(
            solve_kernel,
            tiles=tiles,
            slots=slots,
            total_rows=total_rows,
            total_samples=samples * devices,
        ),
        out_shape=(shape((rank, tiles * LANES), f32), shape((devices, 8, LANES), f32)),
        in_specs=[VMEM],
        out_specs=(VMEM, VMEM),
        name="solve",
    )(received)
    all_sums = lax.all_to_all(sums, "row", split_axis=0, concat_axis=0, tiled=True)
    factor_new, scales = pl.pallas_call(
        functools.partial(scale_kernel, total_rows=total_rows),
        out_shape=(shape((rank, tiles * LANES), jnp.bfloat16), shape((1, rank), f32)),
        in_specs=[VMEM, VMEM],
        out_specs=(VMEM, VMEM),
        name="scale",
    )(all_sums, update)
    return factor_new, scales.reshape(rank)


def solution(mesh):
    in_specs = (
        P(None, ("groups", "row")),
        P(None, ("groups", "row")),
        P(("groups", "row")),
        P(None, ("groups", "row"), None),
        P(("groups", "row")),
        P(("groups", "row"), None, None, None, None),
        P(("groups", "row"), None, None, None),
        P(("groups", "row"), None, None, None),
    )
    out_specs = (P(None, ("groups", "row")), P("groups"))
    return jax.shard_map(shards, mesh=mesh, in_specs=in_specs, out_specs=out_specs, check_vma=False)
```
